32 devices in a mesh: dom: 8 (over y, x, core), rep: 4 (over z).
Axes of the slice: x: 2, y: 2, z: 4, core: 2. Of those that a mesh axis runs over, the one named last changes fastest.
Arguments:
- hop_feats: bfloat16 [3, 65536, 128], P(None, ('dom', 'rep')), may hold values from -6 to 6
- adj_local: bfloat16 [512, 12, 128, 128], P(('dom', 'rep')), may hold values from -0.125 to 0.125
- local_cols: int32 [512, 12], P(('dom', 'rep')), may hold values from 0 to 15
- adj_halo: bfloat16 [512, 4, 128, 128], P(('dom', 'rep')), may hold values from -0.125 to 0.125
- halo_cols: int32 [512, 4], P(('dom', 'rep')), may hold values from 0 to 3
- boundary_rows: int32 [32, 512], P(('dom', 'rep')), may hold values from 0 to 2047
- train_ids: int32 [32, 2048], P(('dom', 'rep')), may hold values from 0 to 2047, as said below
- shuffle: int32 [32, 2048], P(('dom', 'rep')), may hold values from 0 to 2047, as said below
- labels: int32 [65536], P(('dom', 'rep')), may hold values from 0 to 171
- labelled: int32 [65536], P(('dom', 'rep')), may hold values from 0 to 1
- w_first: bfloat16 [512, 1024], P(None, 'rep'), may hold values from -1 to 1
- w_second: bfloat16 [1024, 172], P('rep'), may hold values from -2 to 2
Outputs:
- next_hop: bfloat16 [65536, 128], P(('dom', 'rep'))
- batch_loss: float32 [32, 32], P(('dom', 'rep'))
- grad_first: float32 [512, 1024], P('dom', 'rep')
- grad_second: float32 [1024, 172], P('rep')
The draws below stay inside these ranges and needn't reach their ends.
Inputs may be any that keep to these rules, and one draw needn't show every extreme that they name: `local_cols`: local tile indices of the partition's own row tiles. `halo_cols`: indices of received boundary tiles. `boundary_rows`: rows of the sending partition itself. `train_ids`: rows of the partition itself. `shuffle`: each row is a permutation of 0 .. 2047.
All inputs are finite; a program needn't handle non-finite values.
Results may differ from the reference program's by a relative error of at most 0.005.
The reference program's roundings to bfloat16 on the way count: a program that leaves them out, or rounds other values in their place, can miss the bound.
Values may be sent and summed in bfloat16 or wider, within the bound.
A program may use at most 128 MiB of HBM per device.

```python
import math
import jax
import jax.numpy as jnp
from jax import lax

D_FEAT = 128
HIDDEN_UNITS = 1024
CLASSES = 172
TILE = 128
RT = 16
KL = 12
KH = 4
HALO_TILES = 4
SLOTS = 2048
NODES = 65536
N_DOM = 8
N_REP = 4
DEVICES = 32


def slot_parts(key):
    train_ids = jax.random.randint(jax.random.fold_in(key, 11), (DEVICES, SLOTS), 0, RT * TILE)
    row_keys = jax.random.split(jax.random.fold_in(key, 12), DEVICES)
    shuffle = jax.vmap(lambda one_key: jax.random.permutation(one_key, SLOTS))(row_keys).astype(jnp.int32)
    return (train_ids.astype(jnp.int32), shuffle)


def draw_hop_feats(key, part):
    base = jnp.clip(jax.random.normal(jax.random.fold_in(key, 1), (3, NODES, D_FEAT), jnp.float32), -6.0, 6.0)
    return base.astype(jnp.bfloat16)


def draw_w_first(key, part):
    width = 4 * D_FEAT
    scale = 1.0 / math.sqrt(width)
    base = jnp.clip(jax.random.normal(jax.random.fold_in(key, 4), (width, HIDDEN_UNITS), jnp.float32), -6.0, 6.0) * scale
    return base.astype(jnp.bfloat16)


def draw_w_second(key, part):
    scale = 1.0 / math.sqrt(HIDDEN_UNITS)
    base = jnp.clip(jax.random.normal(jax.random.fold_in(key, 5), (HIDDEN_UNITS, CLASSES), jnp.float32), -6.0, 6.0) * scale
    return base.astype(jnp.bfloat16)


def draw_train_ids(key, part):
    return slot_parts(key)[0]


def draw_shuffle(key, part):
    return slot_parts(key)[1]


def draw_labelled(key, part):
    train_ids, shuffle = slot_parts(key)
    base = (jax.random.randint(jax.random.fold_in(key, 13), (NODES,), 0, 3) < 2).astype(jnp.int32)
    bases = jnp.arange(DEVICES, dtype=jnp.int32)[:, None] * (RT * TILE)
    order = bases + jnp.take_along_axis(train_ids, shuffle, axis=1)
    per = SLOTS // DEVICES
    batches = jnp.transpose(order.reshape(DEVICES, DEVICES, per), (1, 0, 2)).reshape(DEVICES, SLOTS)
    empty = jax.random.randint(jax.random.fold_in(key, 14), (2,), 0, DEVICES)
    cleared = batches[empty].reshape(-1)
    return base.at[cleared].set(0)


def touch_ends(entries, rng, least, largest):
    extent = entries.shape
    index_at = [jax.random.randint(jax.random.fold_in(rng, axis), (), 0, extent[axis]) for axis in range(len(extent))]
    entries = entries.at[tuple(index_at)].set(least)
    longest = extent.index(max(extent))
    index_at[longest] = (index_at[longest] + 1) % extent[longest]
    return entries.at[tuple(index_at)].set(largest)


def steps_of(rng, dims, pieces, least, largest):
    def one(axis_at, parts):
        draws = jax.random.uniform(jax.random.fold_in(jax.random.fold_in(rng, 6), axis_at), (parts,), jnp.float32, least / len(pieces), largest / len(pieces))
        return jnp.repeat(jnp.exp(draws), dims[axis_at] // parts).reshape((-1,) + (1,) * (len(dims) - axis_at - 1))

    gain = one(*pieces[0])
    for cut in pieces[1:]:
        gain = gain * one(*cut)
    return gain


def normal_values(key, extent, scale, most, shards=(), held_as=jnp.bfloat16):
    values = scale * jax.random.normal(key, extent, jnp.float32)
    if shards:
        values = values * steps_of(key, extent, shards, -0.22, 0.18)
    return jnp.clip(values, -most, most).astype(held_as)


def setup_inputs(seed: int = 0) -> dict:
    key_list = jax.random.split(jax.random.key(seed), 13)
    return {
        "hop_feats": draw_hop_feats(jax.random.fold_in(key_list[12], 71), 0),
        "adj_local": normal_values(key_list[1], (NODES // TILE, KL, TILE, TILE), (TILE * (KL + KH)) ** -0.5, 0.125, ((0, 32),)),
        "local_cols": touch_ends(jax.random.randint(key_list[2], (NODES // TILE, KL), 0, RT), jax.random.fold_in(key_list[2], 1), 0, RT - 1).astype(jnp.int32),
        "adj_halo": normal_values(key_list[3], (NODES // TILE, KH, TILE, TILE), (TILE * (KL + KH)) ** -0.5, 0.125, ((0, 32),)),
        "halo_cols": touch_ends(jax.random.randint(key_list[4], (NODES // TILE, KH), 0, HALO_TILES), jax.random.fold_in(key_list[4], 1), 0, HALO_TILES - 1).astype(jnp.int32),
        "boundary_rows": touch_ends(jax.random.randint(key_list[5], (DEVICES, HALO_TILES * TILE), 0, RT * TILE), jax.random.fold_in(key_list[5], 1), 0, (RT * TILE) - 1).astype(jnp.int32),
        "train_ids": draw_train_ids(jax.random.fold_in(key_list[12], 71), 0),
        "shuffle": draw_shuffle(jax.random.fold_in(key_list[12], 71), 0),
        "labels": touch_ends(jax.random.randint(key_list[8], (NODES,), 0, CLASSES), jax.random.fold_in(key_list[8], 1), 0, CLASSES - 1).astype(jnp.int32),
        "labelled": draw_labelled(jax.random.fold_in(key_list[12], 71), 0),
        "w_first": draw_w_first(jax.random.fold_in(key_list[12], 71), 0),
        "w_second": draw_w_second(jax.random.fold_in(key_list[12], 71), 0),
    }


def loss_head(logits, targets, weights_row):
    row_max = lax.optimization_barrier(jnp.max(logits, axis=1, keepdims=True))
    expos = jnp.exp(logits - row_max)
    totals = lax.optimization_barrier(jnp.sum(expos, axis=1, keepdims=True))
    classes = lax.broadcasted_iota(jnp.int32, logits.shape, 1)
    onehot = (classes == targets[:, None]).astype(jnp.float32)
    cross = jnp.log(totals[:, 0]) + row_max[:, 0] - lax.optimization_barrier(jnp.sum(onehot * logits, axis=1))
    count = jnp.maximum(jnp.sum(weights_row), 1.0)
    dlogits = ((expos / totals - onehot) * (weights_row / count)[:, None]).astype(jnp.bfloat16)
    return (cross, dlogits)

def source_losses(cross, weights_row, groups):
    masks = weights_row.reshape(groups, -1)
    sums = lax.optimization_barrier(jnp.sum(masks * cross.reshape(groups, -1), axis=1))
    return sums / jnp.maximum(lax.optimization_barrier(jnp.sum(masks, axis=1)), 1.0)

def batch_norm(pre):
    center = pre - lax.optimization_barrier(jnp.mean(pre, axis=-2, keepdims=True))
    rstd = lax.rsqrt(lax.optimization_barrier(jnp.mean(center * center, axis=-2, keepdims=True)) + 1e-05)
    return (center * rstd, rstd)

def norm_back(grad, normed, rstd):
    mean_grad = lax.optimization_barrier(jnp.mean(grad, axis=-2, keepdims=True))
    mean_proj = lax.optimization_barrier(jnp.mean(grad * normed, axis=-2, keepdims=True))
    return (grad - mean_grad - normed * mean_proj) * rstd

def reference(hop_feats, adj_local, local_cols, adj_halo, halo_cols, boundary_rows, train_ids, shuffle, labels, labelled, w_first, w_second):
    devices = N_DOM * N_REP
    rows = RT * TILE
    share = HALO_TILES * TILE // devices
    hop_two = hop_feats[2]
    bases = jnp.arange(devices, dtype=jnp.int32)[:, None] * rows
    sources = (bases + boundary_rows).reshape(devices, devices, share)
    halo_ids = jnp.transpose(sources, (1, 0, 2)).reshape(devices, devices * share)
    loc_tiles = adj_local.reshape(devices, RT, KL, TILE, TILE)
    loc_cols = local_cols.reshape(devices, RT, KL)
    far_tiles = adj_halo.reshape(devices, RT, KH, TILE, TILE)
    far_cols = halo_cols.reshape(devices, RT, KH)

    def one_part(part):
        own = lax.dynamic_slice_in_dim(hop_two, part * rows, rows, 0)
        own = own.reshape(RT, TILE, D_FEAT).astype(jnp.float32)
        halo = hop_two[halo_ids[part]].reshape(HALO_TILES, TILE, D_FEAT).astype(jnp.float32)
        summed = jnp.einsum('ikab,ikbc->iac', loc_tiles[part].astype(jnp.float32), own[loc_cols[part]])
        summed = summed + jnp.einsum('ikab,ikbc->iac', far_tiles[part].astype(jnp.float32), halo[far_cols[part]])
        return summed.reshape(rows, D_FEAT).astype(jnp.bfloat16)
    next_hop = lax.map(one_part, jnp.arange(devices, dtype=jnp.int32)).reshape(devices * rows, D_FEAT)
    order = bases + jnp.take_along_axis(train_ids, shuffle, axis=1)
    per = SLOTS // devices
    batches = jnp.transpose(order.reshape(devices, devices, per), (1, 0, 2)).reshape(devices, SLOTS)
    allfeat = jnp.concatenate([hop_feats[0], hop_feats[1], hop_feats[2], next_hop], axis=1)

    def one_batch(carry, node_ids):
        grad_one, grad_two = carry
        inputs = allfeat[node_ids]
        targets = labels[node_ids]
        weights_row = labelled[node_ids].astype(jnp.float32)
        hidden_pre = jnp.dot(inputs, w_first, preferred_element_type=jnp.float32)
        normed, rstd = batch_norm(hidden_pre)
        hidden = jnp.maximum(normed, 0.0).astype(jnp.bfloat16)
        logits = jnp.dot(hidden, w_second, preferred_element_type=jnp.float32)
        cross, dlogits = loss_head(logits, targets, weights_row)
        loss = source_losses(cross, weights_row, devices)
        grad_two = grad_two + jnp.dot(hidden.T, dlogits, preferred_element_type=jnp.float32)
        dhidden = jnp.dot(dlogits, w_second.T, preferred_element_type=jnp.float32)
        masked = jnp.where(normed > 0, dhidden, 0.0)
        dpre = norm_back(masked, normed, rstd).astype(jnp.bfloat16)
        grad_one = grad_one + jnp.dot(inputs.T, dpre, preferred_element_type=jnp.float32)
        return ((grad_one, grad_two), loss)
    start = (jnp.zeros((4 * D_FEAT, HIDDEN_UNITS), jnp.float32), jnp.zeros((HIDDEN_UNITS, CLASSES), jnp.float32))
    (grad_first, grad_second), batch_loss = lax.scan(one_batch, start, batches)
    return (next_hop, batch_loss, grad_first, grad_second)
```

```python
import functools

import jax
import jax.numpy as jnp
from jax import lax
from jax.experimental import pallas as pl
from jax.experimental.pallas import tpu as pltpu
from jax.sharding import PartitionSpec as P

F32 = jnp.float32
BF16 = jnp.bfloat16
BIG = 60 * 1024 * 1024


def where_am_i(ndom, nrep):
    return lax.axis_index("dom") * nrep + lax.axis_index("rep")


def enter(me, n, nrep):
    barrier = pltpu.get_barrier_semaphore()

    def greet(o, carry):
        peer = lax.rem(me + o, n)
        pl.semaphore_signal(barrier, inc=1, device_id=(peer // nrep, lax.rem(peer, nrep)),
                            device_id_type=pl.DeviceIdType.MESH)
        return carry

    lax.fori_loop(1, n, greet, 0)
    pl.semaphore_wait(barrier, n - 1)


def spread(me, n, nrep, src_at, dst, send_sem, recv_sem):
    def copy(o):
        peer = lax.rem(me + o, n)
        return pltpu.make_async_remote_copy(
            src_ref=src_at(peer), dst_ref=dst.at[me],
            send_sem=send_sem.at[o], recv_sem=recv_sem.at[o],
            device_id=(peer // nrep, lax.rem(peer, nrep)),
            device_id_type=pl.DeviceIdType.MESH)

    def start(o, carry):
        copy(o).start()
        return carry

    def finish(o, carry):
        copy(o).wait()
        return carry

    return (lambda: lax.fori_loop(1, n, start, 0)), (lambda: lax.fori_loop(1, n, finish, 0))


def comm_call(kernel, outs, scratch, name, cid, *args):
    return pl.pallas_call(
        kernel,
        out_shape=outs,
        in_specs=[pl.BlockSpec(memory_space=pltpu.VMEM)] * len(args),
        out_specs=jax.tree.map(lambda _: pl.BlockSpec(memory_space=pltpu.VMEM), outs),
        scratch_shapes=scratch,
        compiler_params=pltpu.CompilerParams(collective_id=cid, has_side_effects=True),
        name=name,
    )(*args)


def dma_sems(n, count):
    return [pltpu.SemaphoreType.DMA((n,))] * count


def halo_kernel(ndom, nrep, src, out, buf, ssem, rsem):
    n = ndom * nrep
    me = where_am_i(ndom, nrep)
    enter(me, n, nrep)
    start, finish = spread(me, n, nrep, lambda p: src.at[p], buf, ssem, rsem)
    start()
    buf[me] = src[me]
    finish()
    out[...] = buf[...]


def stats_kernel(ndom, nrep, forward, chunk, src, out, extra, recv, gath, s1, r1, s2, r2):
    n = ndom * nrep
    me = where_am_i(ndom, nrep)
    enter(me, n, nrep)
    start, finish = spread(me, n, nrep, lambda p: src.at[p], recv, s1, r1)
    start()
    recv[me] = src[me]
    finish()
    third = src.shape[1] // 3
    got = recv[...]
    first = jnp.sum(got[:, :third], axis=0)
    second = jnp.sum(got[:, third:2 * third], axis=0)
    if forward:
        mu = first * (1.0 / n)
        off = got[:, :third] - mu[None]
        m2 = second + chunk * jnp.sum(off * off, axis=0)
        rstd = lax.rsqrt(m2 * (1.0 / (n * chunk)) + 1e-05)
        count = jnp.maximum(jnp.sum(got[:, 2 * third:], axis=0), 1.0)
        result = jnp.concatenate([mu, rstd, count], axis=0)
        extra[...] = jnp.zeros_like(extra)
    else:
        scale = 1.0 / (n * chunk)
        result = jnp.concatenate([first * scale, second * scale], axis=0)
        extra[...] = got[:, 2 * third:2 * third + 8]
    gath[me] = result
    start, finish = spread(me, n, nrep, lambda p: gath.at[me], gath, s2, r2)
    start()
    finish()
    out[...] = gath[...]


def grads_kernel(ndom, nrep, split, src, out1, out2, recv, gath, s1, r1, s2, r2):
    n = ndom * nrep
    me = where_am_i(ndom, nrep)
    dom, rep = lax.axis_index("dom"), lax.axis_index("rep")
    enter(me, n, nrep)
    start, finish = spread(me, n, nrep, lambda p: src.at[p], recv, s1, r1)
    start()
    recv[me] = src[me]
    finish()

    def add(q, total):
        return total + recv[q].astype(F32)

    total = lax.fori_loop(1, n, add, recv[0].astype(F32))
    out1[...] = total[:split]
    gath[dom] = total[split:]

    def copy(o):
        peer = lax.rem(dom + o, ndom)
        return pltpu.make_async_remote_copy(
            src_ref=gath.at[dom], dst_ref=gath.at[dom],
            send_sem=s2.at[o], recv_sem=r2.at[o], device_id=(peer, rep),
            device_id_type=pl.DeviceIdType.MESH)

    for o in range(1, ndom):
        copy(o).start()
    for o in range(1, ndom):
        copy(o).wait()
    out2[...] = gath[...]


def hop_kernel(kl, kh, lcols, hcols, adj_l, adj_h, own, halo, out):
    i = pl.program_id(0)
    left = jnp.concatenate([adj_l[0, k] for k in range(kl)] + [adj_h[0, k] for k in range(kh)], axis=1)
    right = jnp.concatenate(
        [own[lcols[i, k]] for k in range(kl)] + [halo[hcols[i, k]] for k in range(kh)], axis=0)
    out[0] = jnp.dot(left, right, preferred_element_type=F32).astype(BF16)


def pre_kernel(chunk, shuf, ids, feats, hop, aux, w1, x_out, z_out, aux_out, st_out):
    rows = shuf.shape[0]
    slots = ids.shape[0]
    width = feats.shape[2]
    lanes = lax.broadcasted_iota(jnp.int32, (rows, slots), 1)
    pick = (lanes == shuf[...]).astype(F32).astype(BF16)
    two = jnp.dot(pick, ids[...], preferred_element_type=F32)
    order = (two[:, 0:1] * 256.0 + two[:, 1:2]).astype(jnp.int32)
    nodes = feats.shape[1]
    lanes = lax.broadcasted_iota(jnp.int32, (rows, nodes), 1)
    pick = (lanes == order).astype(F32).astype(BF16)
    whole = jnp.concatenate([feats[0], feats[1], feats[2], hop[...], aux[...]], axis=1)
    got = jnp.dot(pick, whole, preferred_element_type=F32)
    x = got[:, :4 * width].astype(BF16)
    x_out[...] = x
    tags = got[:, 4 * width:]
    aux_out[...] = tags
    z = jnp.concatenate(
        [jnp.dot(x, w1[r], preferred_element_type=F32) for r in range(w1.shape[0])], axis=1)
    z_out[...] = z
    groups = rows // chunk
    z3 = z.reshape(groups, chunk, z.shape[1])
    mean = jnp.sum(z3, axis=1, keepdims=True) * (1.0 / chunk)
    off = z3 - mean
    st_out[:, 0:1] = mean
    st_out[:, 1:2] = jnp.sum(off * off, axis=1, keepdims=True)
    count = jnp.sum(tags[:, 1:2].reshape(groups, chunk, 1), axis=1, keepdims=True)
    st_out[:, 2:3] = jnp.broadcast_to(count, mean.shape)


def head_kernel(chunk, z_ref, aux, st, w2, dl_out, g2_out, gs_out):
    rows, hidden_units = z_ref.shape
    groups = rows // chunk
    stats = st[...]
    z3 = z_ref[...].reshape(groups, chunk, hidden_units)
    normed = ((z3 - stats[:, 0:1]) * stats[:, 1:2]).reshape(rows, hidden_units)
    hidden = jnp.maximum(normed, 0.0).astype(BF16)
    second = w2[...]
    logits = jnp.dot(hidden, second, preferred_element_type=F32)
    row_max = jnp.max(logits, axis=1, keepdims=True)
    expos = jnp.exp(logits - row_max)
    totals = jnp.sum(expos, axis=1, keepdims=True)
    target = aux[:, 0:1].astype(jnp.int32)
    mark = aux[:, 1:2]
    onehot = (lax.broadcasted_iota(jnp.int32, logits.shape, 1) == target).astype(F32)
    cross = jnp.log(totals) + row_max - jnp.sum(onehot * logits, axis=1, keepdims=True)
    count = jnp.broadcast_to(stats[:, 2:3, 0:1], (groups, chunk, 1)).reshape(rows, 1)
    dlogits = ((expos / totals - onehot) * (mark / count)).astype(BF16)
    dl_out[...] = dlogits

    @pl.when(pl.program_id(0) == 0)
    def _():
        g2_out[...] = jnp.zeros_like(g2_out)

    g2_out[...] += lax.dot_general(hidden, dlogits, (((0,), (0,)), ((), ())), preferred_element_type=F32)
    back = lax.dot_general(dlogits, second, (((1,), (1,)), ((), ())), preferred_element_type=F32)
    masked = jnp.where(normed > 0, back, 0.0)
    gs_out[:, 0:1] = jnp.sum(masked.reshape(groups, chunk, hidden_units), axis=1, keepdims=True)
    gs_out[:, 1:2] = jnp.sum((masked * normed).reshape(groups, chunk, hidden_units), axis=1, keepdims=True)
    weighted = jnp.sum((mark * cross).reshape(groups, chunk, 1), axis=1, keepdims=True)
    own_count = jnp.sum(mark.reshape(groups, chunk, 1), axis=1, keepdims=True)
    loss = weighted / jnp.maximum(own_count, 1.0)
    gs_out[:, 2:3] = jnp.broadcast_to(loss, (groups, 1, hidden_units))


def tail_kernel(chunk, z_ref, x_ref, st, gm, w2, dl, g1_out):
    rows, hidden_units = z_ref.shape
    groups = rows // chunk
    stats = st[...]
    means = gm[...]
    z3 = z_ref[...].reshape(groups, chunk, hidden_units)
    rstd = stats[:, 1:2]
    normed = (z3 - stats[:, 0:1]) * rstd
    back = lax.dot_general(dl[...], w2[...], (((1,), (1,)), ((), ())), preferred_element_type=F32)
    masked = jnp.where(normed > 0, back.reshape(groups, chunk, hidden_units), 0.0)
    dpre = ((masked - means[:, 0:1] - normed * means[:, 1:2]) * rstd).reshape(rows, hidden_units)

    @pl.when(pl.program_id(0) == 0)
    def _():
        g1_out[...] = jnp.zeros_like(g1_out)

    g1_out[...] += lax.dot_general(
        x_ref[...], dpre.astype(BF16), (((0,), (0,)), ((), ())), preferred_element_type=F32)


def whole_spec(shape):
    return pl.BlockSpec(tuple(shape), lambda i: (0,) * len(shape))


def lead_spec(shape):
    return pl.BlockSpec(tuple(shape), lambda i: (i,) + (0,) * (len(shape) - 1))


def gather_rep(shard, nrep, rep):
    slots = jnp.zeros((nrep,) + shard.shape, shard.dtype)
    slots = lax.dynamic_update_slice(slots, shard[None], (rep, 0, 0))
    for o in range(1, nrep):
        moved = lax.ppermute(shard, "rep", [(s, (s + o) % nrep) for s in range(nrep)])
        slots = lax.dynamic_update_slice(slots, moved[None], (lax.rem(rep - o + nrep, nrep), 0, 0))
    return slots


def shards(hop_feats, adj_local, local_cols, adj_halo, halo_cols, boundary_rows, train_ids,
           shuffle, labels, labelled, w_first, w_second):
    ndom, nrep = lax.axis_size("dom"), lax.axis_size("rep")
    n = ndom * nrep
    rep = lax.axis_index("rep")
    row_tiles, kl, tile, _ = adj_local.shape
    kh = adj_halo.shape[1]
    rows, width = hop_feats.shape[1:]
    slots = train_ids.shape[1]
    hidden_units, classes = w_second.shape[0] * nrep, w_second.shape[1]
    chunk = slots // n
    block = 256
    steps = slots // block
    groups = block // chunk
    big = pltpu.CompilerParams(vmem_limit_bytes=BIG)
    sds = jax.ShapeDtypeStruct

    w1 = gather_rep(w_first, nrep, rep)
    w2 = gather_rep(w_second, nrep, rep).reshape(hidden_units, classes)

    hop_two = hop_feats[2]
    pick = (boundary_rows[0][:, None] == lax.broadcasted_iota(jnp.int32, (1, rows), 1)).astype(BF16)
    sent = jnp.dot(pick, hop_two, preferred_element_type=F32).astype(BF16)
    share = sent.shape[0] // n
    sent = sent.reshape(n, share, width)
    halo = comm_call(
        functools.partial(halo_kernel, ndom, nrep), sds(sent.shape, BF16),
        [pltpu.VMEM(sent.shape, BF16)] + dma_sems(n, 2), "halo", 1, sent)
    halo = halo.reshape(-1, tile, width)

    next_hop = pl.pallas_call(
        functools.partial(hop_kernel, kl, kh),
        out_shape=sds((row_tiles, tile, width), BF16),
        grid=(row_tiles,),
        in_specs=[
            pl.BlockSpec(memory_space=pltpu.SMEM), pl.BlockSpec(memory_space=pltpu.SMEM),
            lead_spec((1, kl, tile, tile)), lead_spec((1, kh, tile, tile)),
            whole_spec((row_tiles, tile, width)), whole_spec(halo.shape)],
        out_specs=lead_spec((1, tile, width)),
        compiler_params=big, name="hop",
    )(local_cols, halo_cols, adj_local, adj_halo, hop_two.reshape(row_tiles, tile, width), halo)
    next_hop = next_hop.reshape(rows, width)

    lane = lax.broadcasted_iota(jnp.int32, (1, 128), 1)
    ids = train_ids[0][:, None]
    ids = jnp.where(lane == 0, ids // 256, jnp.where(lane == 1, ids % 256, 0)).astype(F32).astype(BF16)
    aux = jnp.where(lane == 0, labels[:, None], jnp.where(lane == 1, labelled[:, None], 0))
    aux = aux.astype(F32).astype(BF16)
    x, z, tags, stats = pl.pallas_call(
        functools.partial(pre_kernel, chunk),
        out_shape=(sds((slots, 4 * width), BF16), sds((slots, hidden_units), F32),
                   sds((slots, 128), F32), sds((n, 3, hidden_units), F32)),
        grid=(steps,),
        in_specs=[lead_spec((block, 1)), whole_spec((slots, 128)), whole_spec(hop_feats.shape),
                  whole_spec((rows, width)), whole_spec((rows, 128)), whole_spec(w1.shape)],
        out_specs=(lead_spec((block, 4 * width)), lead_spec((block, hidden_units)),
                   lead_spec((block, 128)), lead_spec((groups, 3, hidden_units))),
        compiler_params=big, name="pre",
    )(shuffle[0][:, None], ids, hop_feats, next_hop, aux, w1)

    lines = 3 * hidden_units // 128
    third = lines // 3

    def combine(values, forward, cid):
        out_lines = lines if forward else 2 * third
        return comm_call(
            functools.partial(stats_kernel, ndom, nrep, forward, chunk),
            (sds((n, out_lines, 128), F32), sds((n, 8, 128), F32)),
            [pltpu.VMEM((n, lines, 128), F32), pltpu.VMEM((n, out_lines, 128), F32)] + dma_sems(n, 4),
            "stats_f" if forward else "stats_b", cid, values.reshape(n, lines, 128))

    stats, _ = combine(stats, True, 2)
    stats = stats.reshape(n, 3, hidden_units)

    dlogits, grad_two, gsums = pl.pallas_call(
        functools.partial(head_kernel, chunk),
        out_shape=(sds((slots, classes), BF16), sds((hidden_units, classes), F32),
                   sds((n, 3, hidden_units), F32)),
        grid=(steps,),
        in_specs=[lead_spec((block, hidden_units)), lead_spec((block, 128)),
                  lead_spec((groups, 3, hidden_units)), whole_spec((hidden_units, classes))],
        out_specs=(lead_spec((block, classes)), whole_spec((hidden_units, classes)),
                   lead_spec((groups, 3, hidden_units))),
        compiler_params=big, name="head",
    )(z, tags, stats, w2)

    gmeans, losses = combine(gsums, False, 3)
    gmeans = gmeans.reshape(n, 2, hidden_units)
    loss = losses[:, 0, 0].reshape(1, n)

    grad_one = pl.pallas_call(
        functools.partial(tail_kernel, chunk),
        out_shape=sds((4 * width, hidden_units), F32),
        grid=(steps,),
        in_specs=[lead_spec((block, hidden_units)), lead_spec((block, 4 * width)),
                  lead_spec((groups, 3, hidden_units)), lead_spec((groups, 2, hidden_units)),
                  whole_spec((hidden_units, classes)), lead_spec((block, classes))],
        out_specs=whole_spec((4 * width, hidden_units)),
        compiler_params=big, name="tail",
    )(z, x, stats, gmeans, w2, dlogits)

    own_rows, own_cols = 4 * width // ndom, hidden_units // nrep
    one = grad_one.astype(BF16).reshape(ndom, own_rows, nrep, own_cols).transpose(0, 2, 1, 3)
    one = one.reshape(n, own_rows, own_cols)
    part = hidden_units // n
    two = grad_two.astype(BF16).reshape(nrep, ndom, part, classes).transpose(1, 0, 2, 3)
    two = jnp.pad(two.reshape(n, part, classes), ((0, 0), (0, 0), (0, own_cols - classes)))
    packed = jnp.concatenate([one, two], axis=1)
    first, second = comm_call(
        functools.partial(grads_kernel, ndom, nrep, own_rows),
        (sds((own_rows, own_cols), F32), sds((ndom, part, own_cols), F32)),
        [pltpu.VMEM(packed.shape, BF16), pltpu.VMEM((ndom, part, own_cols), F32)] + dma_sems(n, 4),
        "grads", 4, packed)
    second = second.reshape(ndom * part, own_cols)[:, :classes]
    return (next_hop, loss, first, second)


def solution(mesh):
    both = ("dom", "rep")
    placed = (
        P(None, both, None), P(both, None, None, None), P(both, None), P(both, None, None, None),
        P(both, None), P(both, None), P(both, None), P(both, None), P(both), P(both),
        P(None, "rep"), P("rep", None),
    )
    return jax.shard_map(
        shards, mesh=mesh, in_specs=placed,
        out_specs=(P(both, None), P(both, None), P("dom", "rep"), P("rep", None)),
        check_vma=False,
    )
```

```python
import functools

import jax
import jax.numpy as jnp
from jax import lax
from jax.experimental import pallas as pl
from jax.experimental.pallas import tpu as pltpu
from jax.sharding import PartitionSpec as P

F32 = jnp.float32
BF16 = jnp.bfloat16
BIG = 60 * 1024 * 1024


def where_am_i(ndom, nrep):
    return lax.axis_index("dom") * nrep + lax.axis_index("rep")


def enter(me, n, nrep):
    barrier = pltpu.get_barrier_semaphore()

    def greet(o, carry):
        peer = lax.rem(me + o, n)
        pl.semaphore_signal(barrier, inc=1, device_id=(peer // nrep, lax.rem(peer, nrep)),
                            device_id_type=pl.DeviceIdType.MESH)
        return carry

    lax.fori_loop(1, n, greet, 0)
    pl.semaphore_wait(barrier, n - 1)


def spread(me, n, nrep, src_at, dst, send_sem, recv_sem):
    def copy(o):
        peer = lax.rem(me + o, n)
        return pltpu.make_async_remote_copy(
            src_ref=src_at(peer), dst_ref=dst.at[me],
            send_sem=send_sem.at[o], recv_sem=recv_sem.at[o],
            device_id=(peer // nrep, lax.rem(peer, nrep)),
            device_id_type=pl.DeviceIdType.MESH)

    def start(o, carry):
        copy(o).start()
        return carry

    def finish(o, carry):
        copy(o).wait()
        return carry

    return (lambda: lax.fori_loop(1, n, start, 0)), (lambda: lax.fori_loop(1, n, finish, 0))


def comm_call(kernel, outs, scratch, name, cid, *args):
    return pl.pallas_call(
        kernel,
        out_shape=outs,
        in_specs=[pl.BlockSpec(memory_space=pltpu.VMEM)] * len(args),
        out_specs=jax.tree.map(lambda _: pl.BlockSpec(memory_space=pltpu.VMEM), outs),
        scratch_shapes=scratch,
        compiler_params=pltpu.CompilerParams(collective_id=cid, has_side_effects=True),
        name=name,
    )(*args)


def dma_sems(n, count):
    return [pltpu.SemaphoreType.DMA((n,))] * count


def halo_kernel(ndom, nrep, src, cnt, out, tot, buf, crow, cbuf, ssem, rsem, s2, r2):
    n = ndom * nrep
    me = where_am_i(ndom, nrep)
    crow[0] = cnt[...]
    enter(me, n, nrep)
    start, finish = spread(me, n, nrep, lambda p: src.at[p], buf, ssem, rsem)
    cstart, cfinish = spread(me, n, nrep, lambda p: crow.at[0], cbuf, s2, r2)
    start()
    cstart()
    buf[me] = src[me]
    cbuf[me] = cnt[...]
    finish()
    cfinish()
    out[...] = buf[...]
    tot[...] = jnp.maximum(jnp.sum(cbuf[...], axis=0), 1.0)


def stats_kernel(ndom, nrep, forward, chunk, src, row, out, turned, recv, gath, lrow, lbuf,
                 s1, r1, s2, r2, s3, r3):
    n = ndom * nrep
    me = where_am_i(ndom, nrep)
    if not forward:
        lrow[0] = row[...]
    enter(me, n, nrep)
    start, finish = spread(me, n, nrep, lambda p: src.at[p], recv, s1, r1)
    start()
    lstart, lfinish = spread(me, n, nrep, lambda p: lrow.at[0], lbuf, s3, r3)
    if not forward:
        lstart()
        lbuf[me] = row[...]
    recv[me] = src[me]
    finish()
    half = src.shape[1] // 2
    got = recv[...]
    first = jnp.sum(got[:, :half], axis=0)
    second = jnp.sum(got[:, half:], axis=0)
    scale = 1.0 / (n * chunk)
    if forward:
        mu = first * (1.0 / n)
        off = got[:, :half] - mu[None]
        m2 = second + chunk * jnp.sum(off * off, axis=0)
        result = jnp.concatenate([mu, lax.rsqrt(m2 * scale + 1e-05)], axis=0)
    else:
        result = jnp.concatenate([first * scale, second * scale], axis=0)
    gath[me] = result
    start, finish = spread(me, n, nrep, lambda p: gath.at[me], gath, s2, r2)
    start()
    if forward:
        turned[...] = jnp.zeros_like(turned)
    else:
        lfinish()
        losses = lbuf[...]
        source = lax.broadcasted_iota(jnp.int32, losses.shape, 0)
        lane = lax.broadcasted_iota(jnp.int32, losses.shape, 2)
        mine = jnp.sum(jnp.where(lane == me, losses, 0.0), axis=2, keepdims=True)
        turned[...] = jnp.sum(jnp.where(lane == source, mine, 0.0), axis=0)
    finish()
    out[...] = gath[...]


def grads_kernel(ndom, nrep, cores, split, src, out1, out2, recv0, sum0, recv1, sum1, recv2, gath,
                 s0, r0, s1, r1, s2, r2, s3, r3):
    dom, rep = lax.axis_index("dom"), lax.axis_index("rep")
    me = dom * nrep + rep
    chips = ndom // cores
    chip, core = dom // cores, lax.rem(dom, cores)
    enter(me, ndom * nrep, nrep)

    def to(src_ref, dst_ref, ssem, rsem, peer_dom, peer_rep):
        return pltpu.make_async_remote_copy(
            src_ref=src_ref, dst_ref=dst_ref, send_sem=ssem, recv_sem=rsem,
            device_id=(peer_dom, peer_rep), device_id_type=pl.DeviceIdType.MESH)

    def run(copies):
        for copy in copies:
            copy.start()
        for copy in copies:
            copy.wait()

    other = cores - 1 - core
    run([to(src.at[other, a], recv0.at[a], s0.at[a], r0.at[a], chip * cores + other, rep)
         for a in range(chips)])
    sum0[...] = (src[core].astype(F32) + recv0[...].astype(F32)).astype(BF16)

    def near(o):
        peer = lax.rem(chip + o, chips)
        return to(sum0.at[peer], recv1.at[o - 1], s1.at[o], r1.at[o], peer * cores + core, rep)

    run([near(o) for o in range(1, chips)])
    total = sum0[chip].astype(F32)
    for o in range(1, chips):
        total = total + recv1[o - 1].astype(F32)
    sum1[...] = total.astype(BF16)

    def along(o):
        peer = lax.rem(rep + o, nrep)
        return to(sum1.at[peer], recv2.at[o - 1], s2.at[o], r2.at[o], dom, peer)

    run([along(o) for o in range(1, nrep)])
    total = sum1[rep].astype(F32)
    for o in range(1, nrep):
        total = total + recv2[o - 1].astype(F32)
    out1[...] = total[:split]
    gath[dom] = total[split:]
    run([to(gath.at[dom], gath.at[dom], s3.at[o], r3.at[o], lax.rem(dom + o, ndom), rep)
         for o in range(1, ndom)])
    out2[...] = gath[...]


def hop_kernel(kl, kh, lcols, hcols, adj_l, adj_h, own, halo, out):
    i = pl.program_id(0)
    left = jnp.concatenate([adj_l[0, k] for k in range(kl)] + [adj_h[0, k] for k in range(kh)], axis=1)
    right = jnp.concatenate(
        [own[0, lcols[i, k]] for k in range(kl)] + [halo[hcols[i, k]] for k in range(kh)], axis=0)
    out[0] = jnp.dot(left, right, preferred_element_type=F32).astype(BF16)


def batch_lanes(rows, wide, chunk):
    at = pl.program_id(0) * rows + lax.broadcasted_iota(jnp.int32, (rows, wide), 0)
    return at // chunk == lax.broadcasted_iota(jnp.int32, (rows, wide), 1)


def one_hot(column, count):
    lanes = lax.broadcasted_iota(jnp.int32, (column.shape[0], count), 1)
    return (lanes == column).astype(F32).astype(BF16)


def by_lanes(left, right):
    return lax.dot_general(left, right, (((1,), (1,)), ((), ())), preferred_element_type=F32)


def pick_kernel(chunk, shuf, bound, ids, labels, labelled, feats, x_out, tag_out, sent_out, cnt_out):
    rows = shuf.shape[0]
    nodes = feats.shape[1]
    sent_out[...] = jnp.dot(one_hot(bound[...], nodes), feats[2], preferred_element_type=F32).astype(BF16)
    numbers = ids[...]
    blank = jnp.zeros((6, nodes), F32)
    table = jnp.concatenate(
        [(numbers // 256).astype(F32), (numbers % 256).astype(F32), jnp.zeros((6, ids.shape[1]), F32)], axis=0)
    two = by_lanes(one_hot(shuf[...], ids.shape[1]), table.astype(BF16))
    order = two[:, 0:1] * 256.0 + two[:, 1:2]
    pick = one_hot(order.astype(jnp.int32), nodes)
    whole = jnp.concatenate([feats[0], feats[1], feats[2]], axis=1)
    x_out[...] = jnp.dot(pick, whole, preferred_element_type=F32).astype(BF16)
    marks = jnp.concatenate([labels[...].astype(F32), labelled[...].astype(F32), blank], axis=0)
    tags = by_lanes(pick, marks.astype(BF16))
    tag_out[:, 0:8] = tags
    tag_out[:, 8:9] = order

    @pl.when(pl.program_id(0) == 0)
    def _():
        cnt_out[...] = jnp.zeros_like(cnt_out)

    here = batch_lanes(rows, cnt_out.shape[1], chunk)
    cnt_out[...] += jnp.sum(jnp.where(here, tags[:, 1:2], 0.0), axis=0, keepdims=True)


def store_lines(out, at, value):
    for j in range(value.shape[2] // 128):
        out[:, at + j:at + j + 1] = value[:, :, j * 128:(j + 1) * 128]


def load_lines(ref, at, lines):
    return jnp.concatenate([ref[:, at + j:at + j + 1] for j in range(lines)], axis=2)


def pre_kernel(chunk, x3, tag, hop, w1, x_out, z_out, st_out):
    rows = x3.shape[0]
    order = tag[:, 8:9].astype(jnp.int32)
    got = jnp.dot(one_hot(order, hop.shape[0]), hop[...], preferred_element_type=F32)
    x = jnp.concatenate([x3[...], got.astype(BF16)], axis=1)
    x_out[...] = x
    z = jnp.concatenate(
        [jnp.dot(x, w1[r], preferred_element_type=F32) for r in range(w1.shape[0])], axis=1)
    z_out[...] = z
    z3 = z.reshape(rows // chunk, chunk, z.shape[1])
    mean = jnp.sum(z3, axis=1, keepdims=True) * (1.0 / chunk)
    off = z3 - mean
    store_lines(st_out, 0, mean)
    store_lines(st_out, st_out.shape[1] // 2, jnp.sum(off * off, axis=1, keepdims=True))


def head_kernel(chunk, z_ref, tag, st, counts, own_counts, w2, dl_out, g2_out, gs_out, loss_out):
    rows, hidden_units = z_ref.shape
    groups = rows // chunk
    half = st.shape[1] // 2
    z3 = z_ref[...].reshape(groups, chunk, hidden_units)
    normed = ((z3 - load_lines(st, 0, half)) * load_lines(st, half, half)).reshape(rows, hidden_units)
    hidden = jnp.maximum(normed, 0.0).astype(BF16)
    second = w2[...]
    logits = jnp.dot(hidden, second, preferred_element_type=F32)
    row_max = jnp.max(logits, axis=1, keepdims=True)
    expos = jnp.exp(logits - row_max)
    totals = jnp.sum(expos, axis=1, keepdims=True)
    target = tag[:, 0:1].astype(jnp.int32)
    mark = tag[:, 1:2]
    onehot = (lax.broadcasted_iota(jnp.int32, logits.shape, 1) == target).astype(F32)
    cross = jnp.log(totals) + row_max - jnp.sum(onehot * logits, axis=1, keepdims=True)
    here = batch_lanes(rows, counts.shape[1], chunk)
    count = jnp.sum(jnp.where(here, counts[...], 0.0), axis=1, keepdims=True)
    dlogits = ((expos / totals - onehot) * (mark / count)).astype(BF16)
    dl_out[...] = dlogits

    @pl.when(pl.program_id(0) == 0)
    def _():
        g2_out[...] = jnp.zeros_like(g2_out)
        loss_out[...] = jnp.zeros_like(loss_out)

    loss_out[...] += jnp.sum(jnp.where(here, mark * cross, 0.0), axis=0, keepdims=True)

    @pl.when(pl.program_id(0) == pl.num_programs(0) - 1)
    def _():
        loss_out[...] = loss_out[...] / jnp.maximum(own_counts[...], 1.0)

    g2_out[...] += lax.dot_general(hidden, dlogits, (((0,), (0,)), ((), ())), preferred_element_type=F32)
    masked = jnp.where(normed > 0, by_lanes(dlogits, second), 0.0)
    store_lines(gs_out, 0, jnp.sum(masked.reshape(groups, chunk, hidden_units), axis=1, keepdims=True))
    store_lines(gs_out, half, jnp.sum(
        (masked * normed).reshape(groups, chunk, hidden_units), axis=1, keepdims=True))


def tail_kernel(chunk, ndom, nrep, cores, z_ref, x_ref, st, gm, w2, dl, g2, out, acc):
    rows, hidden_units = z_ref.shape
    groups = rows // chunk
    half = st.shape[1] // 2
    z3 = z_ref[...].reshape(groups, chunk, hidden_units)
    rstd = load_lines(st, half, half)
    normed = (z3 - load_lines(st, 0, half)) * rstd
    back = by_lanes(dl[...], w2[...])
    masked = jnp.where(normed > 0, back.reshape(groups, chunk, hidden_units), 0.0)
    dpre = (masked - load_lines(gm, 0, half) - normed * load_lines(gm, half, half)) * rstd
    dpre = dpre.reshape(rows, hidden_units).astype(BF16)

    @pl.when(pl.program_id(0) == 0)
    def _():
        acc[...] = jnp.zeros_like(acc)

    acc[...] += lax.dot_general(x_ref[...], dpre, (((0,), (0,)), ((), ())), preferred_element_type=F32)

    @pl.when(pl.program_id(0) == pl.num_programs(0) - 1)
    def _():
        high, wide = acc.shape[0] // ndom, acc.shape[1] // nrep
        part, classes = g2.shape[0] // (ndom * nrep), g2.shape[1]
        for d in range(ndom):
            for r in range(nrep):
                first = acc[d * high:(d + 1) * high, r * wide:(r + 1) * wide]
                at = (r * ndom + d) * part
                second = jnp.concatenate(
                    [g2[at:at + part, :], jnp.zeros((part, wide - classes), F32)], axis=1)
                out[d % cores, d // cores, r] = jnp.concatenate([first, second], axis=0).astype(BF16)


def whole_spec(shape):
    return pl.BlockSpec(tuple(shape), lambda i: (0,) * len(shape))


def lead_spec(shape):
    return pl.BlockSpec(tuple(shape), lambda i: (i,) + (0,) * (len(shape) - 1))


def gather_rep(half, ndom, nrep, cores):
    dom, rep = lax.axis_index("dom"), lax.axis_index("rep")
    core = lax.rem(dom, cores)
    slots = jnp.zeros((nrep,) + half.shape, half.dtype)
    slots = lax.dynamic_update_slice(slots, half[None], (rep, 0, 0))
    for o in range(1, nrep):
        moved = lax.ppermute(half, "rep", [(s, (s + o) % nrep) for s in range(nrep)])
        slots = lax.dynamic_update_slice(slots, moved[None], (lax.rem(rep - o + nrep, nrep), 0, 0))
    theirs = lax.ppermute(slots, "dom", [(d, d + 1 - 2 * (d % 2)) for d in range(ndom)])
    both = jnp.zeros((cores,) + slots.shape, slots.dtype)
    both = lax.dynamic_update_slice(both, slots[None], (core, 0, 0, 0))
    return lax.dynamic_update_slice(both, theirs[None], (cores - 1 - core, 0, 0, 0))


def shards(hop_feats, adj_local, local_cols, adj_halo, halo_cols, boundary_rows, train_ids,
           shuffle, labels, labelled, w_first, w_second):
    ndom, nrep = lax.axis_size("dom"), lax.axis_size("rep")
    n = ndom * nrep
    cores = 2
    row_tiles, kl, tile, _ = adj_local.shape
    kh = adj_halo.shape[1]
    rows, width = hop_feats.shape[1:]
    slots = train_ids.shape[1]
    hidden_units, classes = w_second.shape[0] * nrep, w_second.shape[1]
    chunk = slots // n
    block = 256
    steps = slots // block
    groups = block // chunk
    wide = -(-n // 128) * 128
    big = pltpu.CompilerParams(vmem_limit_bytes=BIG)
    sds = jax.ShapeDtypeStruct

    core = lax.rem(lax.axis_index("dom"), cores)
    own_cols = hidden_units // nrep
    h1, h2 = w_first.shape[0] // cores, w_second.shape[0] // cores
    half = jnp.concatenate([
        lax.dynamic_slice(w_first, (core * h1, 0), (h1, own_cols)),
        jnp.pad(lax.dynamic_slice(w_second, (core * h2, 0), (h2, classes)),
                ((0, 0), (0, own_cols - classes)))], axis=0)
    both = gather_rep(half, ndom, nrep, cores)

    sent_block = boundary_rows.shape[1] // steps
    x3, tags, sent, own_counts = pl.pallas_call(
        functools.partial(pick_kernel, chunk),
        out_shape=(sds((slots, 3 * width), BF16), sds((slots, 128), F32),
                   sds((boundary_rows.shape[1], width), BF16), sds((1, wide), F32)),
        grid=(steps,),
        in_specs=[lead_spec((block, 1)), lead_spec((sent_block, 1)), whole_spec((1, slots)),
                  whole_spec((1, rows)), whole_spec((1, rows)), whole_spec(hop_feats.shape)],
        out_specs=(lead_spec((block, 3 * width)), lead_spec((block, 128)),
                   lead_spec((sent_block, width)), whole_spec((1, wide))),
        compiler_params=big, name="pick",
        cost_estimate=pl.CostEstimate(flops=2 * slots * rows * 5 * width, bytes_accessed=4 << 20, transcendentals=0),
    )(shuffle[0][:, None], boundary_rows[0][:, None], train_ids, labels[None], labelled[None], hop_feats)

    sent = sent.reshape(n, -1, width)
    halo, counts = comm_call(
        functools.partial(halo_kernel, ndom, nrep), (sds(sent.shape, BF16), sds((1, wide), F32)),
        [pltpu.VMEM(sent.shape, BF16), pltpu.VMEM((1, 1, wide), F32), pltpu.VMEM((n, 1, wide), F32)]
        + dma_sems(n, 4), "halo", 1, sent, own_counts)
    halo = halo.reshape(-1, tile, width)

    next_hop = pl.pallas_call(
        functools.partial(hop_kernel, kl, kh),
        out_shape=sds((row_tiles, tile, width), BF16),
        grid=(row_tiles,),
        in_specs=[
            pl.BlockSpec(memory_space=pltpu.SMEM), pl.BlockSpec(memory_space=pltpu.SMEM),
            lead_spec((1, kl, tile, tile)), lead_spec((1, kh, tile, tile)),
            pl.BlockSpec((1, row_tiles, tile, width), lambda i: (2, 0, 0, 0)), whole_spec(halo.shape)],
        out_specs=lead_spec((1, tile, width)),
        compiler_params=big, name="hop",
        cost_estimate=pl.CostEstimate(flops=2 * rows * width * tile * (kl + kh), bytes_accessed=9 << 20, transcendentals=0),
    )(local_cols, halo_cols, adj_local, adj_halo, hop_feats.reshape(3, row_tiles, tile, width), halo)
    next_hop = next_hop.reshape(rows, width)

    w1 = both[:, :, :h1].transpose(1, 0, 2, 3).reshape(nrep, cores * h1, own_cols)
    w2 = both[:, :, h1:, :classes].transpose(1, 0, 2, 3).reshape(hidden_units, classes)

    lines = 2 * hidden_units // 128
    x, z, stats = pl.pallas_call(
        functools.partial(pre_kernel, chunk),
        out_shape=(sds((slots, 4 * width), BF16), sds((slots, hidden_units), F32),
                   sds((n, lines, 128), F32)),
        grid=(steps,),
        in_specs=[lead_spec((block, 3 * width)), lead_spec((block, 128)), whole_spec((rows, width)),
                  whole_spec(w1.shape)],
        out_specs=(lead_spec((block, 4 * width)), lead_spec((block, hidden_units)),
                   lead_spec((groups, lines, 128))),
        compiler_params=big, name="pre",
    )(x3, tags, next_hop, w1)

    def combine(values, row, forward, cid):
        return comm_call(
            functools.partial(stats_kernel, ndom, nrep, forward, chunk),
            (sds((n, lines, 128), F32), sds((1, wide), F32)),
            [pltpu.VMEM((n, lines, 128), F32)] * 2
            + [pltpu.VMEM((1, 1, wide), F32), pltpu.VMEM((n, 1, wide), F32)] + dma_sems(n, 6),
            "stats_f" if forward else "stats_b", cid, values, row)

    stats, _ = combine(stats, own_counts, True, 2)

    line_spec = lead_spec((groups, lines, 128))
    dlogits, grad_two, gsums, losses = pl.pallas_call(
        functools.partial(head_kernel, chunk),
        out_shape=(sds((slots, classes), BF16), sds((hidden_units, classes), F32),
                   sds((n, lines, 128), F32), sds((1, wide), F32)),
        grid=(steps,),
        in_specs=[lead_spec((block, hidden_units)), lead_spec((block, 128)), line_spec,
                  whole_spec((1, wide)), whole_spec((1, wide)), whole_spec((hidden_units, classes))],
        out_specs=(lead_spec((block, classes)), whole_spec((hidden_units, classes)), line_spec,
                   whole_spec((1, wide))),
        compiler_params=big, name="head",
    )(z, tags, stats, counts, own_counts, w2)

    gmeans, turned = combine(gsums, losses, False, 3)
    loss = turned[:, :n]

    own_rows, part = 4 * width // ndom, hidden_units // n
    size = (nrep, own_rows + part, own_cols)
    packed = pl.pallas_call(
        functools.partial(tail_kernel, chunk, ndom, nrep, cores),
        out_shape=sds((cores, ndom // cores) + size, BF16),
        grid=(steps,),
        in_specs=[lead_spec((block, hidden_units)), lead_spec((block, 4 * width)), line_spec, line_spec,
                  whole_spec((hidden_units, classes)), lead_spec((block, classes)),
                  whole_spec((hidden_units, classes))],
        out_specs=whole_spec((cores, ndom // cores) + size),
        scratch_shapes=[pltpu.VMEM((4 * width, hidden_units), F32)],
        compiler_params=big, name="tail",
    )(z, x, stats, gmeans, w2, dlogits, grad_two)

    chips = ndom // cores
    first, second = comm_call(
        functools.partial(grads_kernel, ndom, nrep, cores, own_rows),
        (sds((own_rows, own_cols), F32), sds((ndom, part, own_cols), F32)),
        [pltpu.VMEM((chips,) + size, BF16), pltpu.VMEM((chips,) + size, BF16),
         pltpu.VMEM((chips - 1,) + size, BF16), pltpu.VMEM(size, BF16),
         pltpu.VMEM((nrep - 1,) + size[1:], BF16), pltpu.VMEM((ndom, part, own_cols), F32)]
        + dma_sems(chips, 4) + dma_sems(nrep, 2) + dma_sems(ndom, 2),
        "grads", 4, packed)
    second = second.reshape(ndom * part, own_cols)[:, :classes]
    return (next_hop, loss, first, second)


def solution(mesh):
    both = ("dom", "rep")
    placed = (
        P(None, both, None), P(both, None, None, None), P(both, None), P(both, None, None, None),
        P(both, None), P(both, None), P(both, None), P(both, None), P(both), P(both),
        P(None, "rep"), P("rep", None),
    )
    return jax.shard_map(
        shards, mesh=mesh, in_specs=placed,
        out_specs=(P(both, None), P(both, None), P("dom", "rep"), P("rep", None)),
        check_vma=False,
    )
```

```python
import functools

import jax
import jax.numpy as jnp
from jax import lax
from jax.experimental import pallas as pl
from jax.experimental.pallas import tpu as pltpu
from jax.sharding import PartitionSpec as P

F32 = jnp.float32
BF16 = jnp.bfloat16
BIG = 60 * 1024 * 1024


def where_am_i(ndom, nrep):
    return lax.axis_index("dom") * nrep + lax.axis_index("rep")


def enter(me, n, nrep):
    barrier = pltpu.get_barrier_semaphore()

    def greet(o, carry):
        peer = lax.rem(me + o, n)
        pl.semaphore_signal(barrier, inc=1, device_id=(peer // nrep, lax.rem(peer, nrep)),
                            device_id_type=pl.DeviceIdType.MESH)
        return carry

    lax.fori_loop(1, n, greet, 0)
    pl.semaphore_wait(barrier, n - 1)


def spread(me, n, nrep, src_at, dst, send_sem, recv_sem):
    def copy(o):
        peer = lax.rem(me + o, n)
        return pltpu.make_async_remote_copy(
            src_ref=src_at(peer), dst_ref=dst.at[me],
            send_sem=send_sem.at[o], recv_sem=recv_sem.at[o],
            device_id=(peer // nrep, lax.rem(peer, nrep)),
            device_id_type=pl.DeviceIdType.MESH)

    def start(o, carry):
        copy(o).start()
        return carry

    def finish(o, carry):
        copy(o).wait()
        return carry

    return (lambda: lax.fori_loop(1, n, start, 0)), (lambda: lax.fori_loop(1, n, finish, 0))


def comm_call(kernel, outs, scratch, name, cid, *args):
    return pl.pallas_call(
        kernel,
        out_shape=outs,
        in_specs=[pl.BlockSpec(memory_space=pltpu.VMEM)] * len(args),
        out_specs=jax.tree.map(lambda _: pl.BlockSpec(memory_space=pltpu.VMEM), outs),
        scratch_shapes=scratch,
        compiler_params=pltpu.CompilerParams(collective_id=cid, has_side_effects=True),
        name=name,
    )(*args)


def dma_sems(n, count):
    return [pltpu.SemaphoreType.DMA((n,))] * count


def halo_kernel(ndom, nrep, src, cnt, out, tot, buf, crow, cbuf, ssem, rsem, s2, r2):
    n = ndom * nrep
    me = where_am_i(ndom, nrep)
    crow[0] = cnt[...]
    enter(me, n, nrep)
    start, finish = spread(me, n, nrep, lambda p: src.at[p], buf, ssem, rsem)
    cstart, cfinish = spread(me, n, nrep, lambda p: crow.at[0], cbuf, s2, r2)
    start()
    cstart()
    buf[me] = src[me]
    cbuf[me] = cnt[...]
    finish()
    cfinish()
    out[...] = buf[...]
    tot[...] = jnp.maximum(jnp.sum(cbuf[...], axis=0), 1.0)


def stats_kernel(ndom, nrep, forward, chunk, src, row, out, turned, recv, gath, lrow, lbuf,
                 s1, r1, s2, r2, s3, r3):
    n = ndom * nrep
    me = where_am_i(ndom, nrep)
    if not forward:
        lrow[0] = row[...]
    enter(me, n, nrep)
    start, finish = spread(me, n, nrep, lambda p: src.at[p], recv, s1, r1)
    start()
    lstart, lfinish = spread(me, n, nrep, lambda p: lrow.at[0], lbuf, s3, r3)
    if not forward:
        lstart()
        lbuf[me] = row[...]
    recv[me] = src[me]
    finish()
    half = src.shape[1] // 2
    got = recv[...]
    first = jnp.sum(got[:, :half], axis=0)
    second = jnp.sum(got[:, half:], axis=0)
    scale = 1.0 / (n * chunk)
    if forward:
        mu = first * (1.0 / n)
        off = got[:, :half] - mu[None]
        m2 = second + chunk * jnp.sum(off * off, axis=0)
        result = jnp.concatenate([mu, lax.rsqrt(m2 * scale + 1e-05)], axis=0)
    else:
        result = jnp.concatenate([first * scale, second * scale], axis=0)
    gath[me] = result
    start, finish = spread(me, n, nrep, lambda p: gath.at[me], gath, s2, r2)
    start()
    if forward:
        turned[...] = jnp.zeros_like(turned)
    else:
        lfinish()
        losses = lbuf[...]
        source = lax.broadcasted_iota(jnp.int32, losses.shape, 0)
        lane = lax.broadcasted_iota(jnp.int32, losses.shape, 2)
        mine = jnp.sum(jnp.where(lane == me, losses, 0.0), axis=2, keepdims=True)
        turned[...] = jnp.sum(jnp.where(lane == source, mine, 0.0), axis=0)
    finish()
    out[...] = gath[...]


def grads_kernel(ndom, nrep, cores, split, src, out1, out2, recv0, sum0, recv1, sum1, kept, recv2, gath,
                 s0, r0, s1, r1, s2, r2, s3, r3):
    dom, rep = lax.axis_index("dom"), lax.axis_index("rep")
    me = dom * nrep + rep
    chips = ndom // cores
    chip, core = dom // cores, lax.rem(dom, cores)
    enter(me, ndom * nrep, nrep)

    def to(src_ref, dst_ref, ssem, rsem, peer_dom, peer_rep):
        return pltpu.make_async_remote_copy(
            src_ref=src_ref, dst_ref=dst_ref, send_sem=ssem, recv_sem=rsem,
            device_id=(peer_dom, peer_rep), device_id_type=pl.DeviceIdType.MESH)

    def run(copies):
        for copy in copies:
            copy.start()
        for copy in copies:
            copy.wait()

    other = cores - 1 - core
    run([to(src.at[other, a], recv0.at[a], s0.at[a], r0.at[a], chip * cores + other, rep)
         for a in range(chips)])
    sum0[...] = (src[core].astype(F32) + recv0[...].astype(F32)).astype(BF16)

    def near(o):
        peer = lax.rem(chip + o, chips)
        return to(sum0.at[peer], recv1.at[o - 1], s1.at[o], r1.at[o], peer * cores + core, rep)

    run([near(o) for o in range(1, chips)])
    total = src[core, chip].astype(F32) + recv0[chip].astype(F32)
    for o in range(1, chips):
        total = total + recv1[o - 1].astype(F32)
    sum1[...] = total.astype(BF16)
    kept[...] = total

    def along(o):
        peer = lax.rem(rep + o, nrep)
        return to(sum1.at[peer], recv2.at[o - 1], s2.at[o], r2.at[o], dom, peer)

    run([along(o) for o in range(1, nrep)])
    total = kept[rep]
    for o in range(1, nrep):
        total = total + recv2[o - 1].astype(F32)
    out1[...] = total[:split]
    gath[dom] = total[split:]
    run([to(gath.at[dom], gath.at[dom], s3.at[o], r3.at[o], lax.rem(dom + o, ndom), rep)
         for o in range(1, ndom)])
    out2[...] = gath[...]


def hop_kernel(kl, kh, lcols, hcols, adj_l, adj_h, own, halo, out):
    i = pl.program_id(0)
    left = jnp.concatenate([adj_l[0, k] for k in range(kl)] + [adj_h[0, k] for k in range(kh)], axis=1)
    right = jnp.concatenate(
        [own[0, lcols[i, k]] for k in range(kl)] + [halo[hcols[i, k]] for k in range(kh)], axis=0)
    out[0] = jnp.dot(left, right, preferred_element_type=F32).astype(BF16)


def batch_lanes(rows, wide, chunk):
    at = pl.program_id(0) * rows + lax.broadcasted_iota(jnp.int32, (rows, wide), 0)
    return at // chunk == lax.broadcasted_iota(jnp.int32, (rows, wide), 1)


def one_hot(column, count):
    lanes = lax.broadcasted_iota(jnp.int32, (column.shape[0], count), 1)
    return (lanes == column).astype(F32).astype(BF16)


def by_lanes(left, right):
    return lax.dot_general(left, right, (((1,), (1,)), ((), ())), preferred_element_type=F32)


def pick_kernel(chunk, shuf, bound, ids, labels, labelled, feats, x_out, tag_out, sent_out, cnt_out):
    rows = shuf.shape[0]
    nodes = feats.shape[1]
    sent_out[...] = jnp.dot(one_hot(bound[...], nodes), feats[2], preferred_element_type=F32).astype(BF16)
    numbers = ids[...]
    blank = jnp.zeros((6, nodes), F32)
    table = jnp.concatenate(
        [(numbers // 256).astype(F32), (numbers % 256).astype(F32), jnp.zeros((6, ids.shape[1]), F32)], axis=0)
    two = by_lanes(one_hot(shuf[...], ids.shape[1]), table.astype(BF16))
    order = two[:, 0:1] * 256.0 + two[:, 1:2]
    pick = one_hot(order.astype(jnp.int32), nodes)
    whole = jnp.concatenate([feats[0], feats[1], feats[2]], axis=1)
    x_out[...] = jnp.dot(pick, whole, preferred_element_type=F32).astype(BF16)
    marks = jnp.concatenate([labels[...].astype(F32), labelled[...].astype(F32), blank], axis=0)
    tags = by_lanes(pick, marks.astype(BF16))
    tag_out[:, 0:8] = tags
    tag_out[:, 8:9] = order

    @pl.when(pl.program_id(0) == 0)
    def _():
        cnt_out[...] = jnp.zeros_like(cnt_out)

    here = batch_lanes(rows, cnt_out.shape[1], chunk)
    cnt_out[...] += jnp.sum(jnp.where(here, tags[:, 1:2], 0.0), axis=0, keepdims=True)


def store_lines(out, at, value):
    for j in range(value.shape[2] // 128):
        out[:, at + j:at + j + 1] = value[:, :, j * 128:(j + 1) * 128]


def load_lines(ref, at, lines):
    return jnp.concatenate([ref[:, at + j:at + j + 1] for j in range(lines)], axis=2)


def pre_kernel(chunk, x3, tag, hop, w1, x_out, z_out, st_out):
    rows = x3.shape[0]
    order = tag[:, 8:9].astype(jnp.int32)
    got = jnp.dot(one_hot(order, hop.shape[0]), hop[...], preferred_element_type=F32)
    x = jnp.concatenate([x3[...], got.astype(BF16)], axis=1)
    x_out[...] = x
    z = jnp.concatenate(
        [jnp.dot(x, w1[r], preferred_element_type=F32) for r in range(w1.shape[0])], axis=1)
    z_out[...] = z
    z3 = z.reshape(rows // chunk, chunk, z.shape[1])
    mean = jnp.sum(z3, axis=1, keepdims=True) * (1.0 / chunk)
    off = z3 - mean
    store_lines(st_out, 0, mean)
    store_lines(st_out, st_out.shape[1] // 2, jnp.sum(off * off, axis=1, keepdims=True))


def head_kernel(chunk, z_ref, tag, st, counts, own_counts, w2, dl_out, g2_out, gs_out, loss_out):
    rows, hidden_units = z_ref.shape
    groups = rows // chunk
    half = st.shape[1] // 2
    z3 = z_ref[...].reshape(groups, chunk, hidden_units)
    normed = ((z3 - load_lines(st, 0, half)) * load_lines(st, half, half)).reshape(rows, hidden_units)
    hidden = jnp.maximum(normed, 0.0).astype(BF16)
    second = w2[...]
    logits = jnp.dot(hidden, second, preferred_element_type=F32)
    row_max = jnp.max(logits, axis=1, keepdims=True)
    expos = jnp.exp(logits - row_max)
    totals = jnp.sum(expos, axis=1, keepdims=True)
    target = tag[:, 0:1].astype(jnp.int32)
    mark = tag[:, 1:2]
    onehot = (lax.broadcasted_iota(jnp.int32, logits.shape, 1) == target).astype(F32)
    cross = jnp.log(totals) + row_max - jnp.sum(onehot * logits, axis=1, keepdims=True)
    here = batch_lanes(rows, counts.shape[1], chunk)
    count = jnp.sum(jnp.where(here, counts[...], 0.0), axis=1, keepdims=True)
    dlogits = ((expos / totals - onehot) * (mark / count)).astype(BF16)
    dl_out[...] = dlogits

    @pl.when(pl.program_id(0) == 0)
    def _():
        g2_out[...] = jnp.zeros_like(g2_out)
        loss_out[...] = jnp.zeros_like(loss_out)

    loss_out[...] += jnp.sum(jnp.where(here, mark * cross, 0.0), axis=0, keepdims=True)

    @pl.when(pl.program_id(0) == pl.num_programs(0) - 1)
    def _():
        loss_out[...] = loss_out[...] / jnp.maximum(own_counts[...], 1.0)

    g2_out[...] += lax.dot_general(hidden, dlogits, (((0,), (0,)), ((), ())), preferred_element_type=F32)
    masked = jnp.where(normed > 0, by_lanes(dlogits, second), 0.0)
    store_lines(gs_out, 0, jnp.sum(masked.reshape(groups, chunk, hidden_units), axis=1, keepdims=True))
    store_lines(gs_out, half, jnp.sum(
        (masked * normed).reshape(groups, chunk, hidden_units), axis=1, keepdims=True))


def tail_kernel(chunk, ndom, nrep, cores, z_ref, x_ref, st, gm, w2, dl, g2, out, acc):
    rows, hidden_units = z_ref.shape
    groups = rows // chunk
    half = st.shape[1] // 2
    z3 = z_ref[...].reshape(groups, chunk, hidden_units)
    rstd = load_lines(st, half, half)
    normed = (z3 - load_lines(st, 0, half)) * rstd
    back = by_lanes(dl[...], w2[...])
    masked = jnp.where(normed > 0, back.reshape(groups, chunk, hidden_units), 0.0)
    dpre = (masked - load_lines(gm, 0, half) - normed * load_lines(gm, half, half)) * rstd
    dpre = dpre.reshape(rows, hidden_units).astype(BF16)

    @pl.when(pl.program_id(0) == 0)
    def _():
        acc[...] = jnp.zeros_like(acc)

    acc[...] += lax.dot_general(x_ref[...], dpre, (((0,), (0,)), ((), ())), preferred_element_type=F32)

    @pl.when(pl.program_id(0) == pl.num_programs(0) - 1)
    def _():
        high, wide = acc.shape[0] // ndom, acc.shape[1] // nrep
        part, classes = g2.shape[0] // (ndom * nrep), g2.shape[1]
        for d in range(ndom):
            for r in range(nrep):
                first = acc[d * high:(d + 1) * high, r * wide:(r + 1) * wide]
                at = (r * ndom + d) * part
                second = jnp.concatenate(
                    [g2[at:at + part, :], jnp.zeros((part, wide - classes), F32)], axis=1)
                out[d % cores, d // cores, r] = jnp.concatenate([first, second], axis=0).astype(BF16)


def whole_spec(shape):
    return pl.BlockSpec(tuple(shape), lambda i: (0,) * len(shape))


def lead_spec(shape):
    return pl.BlockSpec(tuple(shape), lambda i: (i,) + (0,) * (len(shape) - 1))


def send_rep(half, nrep):
    return [lax.ppermute(half, "rep", [(s, (s + o) % nrep) for s in range(nrep)]) for o in range(1, nrep)]


def gather_rep(half, arrived, ndom, nrep, cores):
    dom, rep = lax.axis_index("dom"), lax.axis_index("rep")
    core = lax.rem(dom, cores)
    slots = jnp.zeros((nrep,) + half.shape, half.dtype)
    slots = lax.dynamic_update_slice(slots, half[None], (rep, 0, 0))
    for o in range(1, nrep):
        slots = lax.dynamic_update_slice(slots, arrived[o - 1][None], (lax.rem(rep - o + nrep, nrep), 0, 0))
    theirs = lax.ppermute(slots, "dom", [(d, d + 1 - 2 * (d % 2)) for d in range(ndom)])
    both = jnp.zeros((cores,) + slots.shape, slots.dtype)
    both = lax.dynamic_update_slice(both, slots[None], (core, 0, 0, 0))
    return lax.dynamic_update_slice(both, theirs[None], (cores - 1 - core, 0, 0, 0))


def shards(hop_feats, adj_local, local_cols, adj_halo, halo_cols, boundary_rows, train_ids,
           shuffle, labels, labelled, w_first, w_second):
    ndom, nrep = lax.axis_size("dom"), lax.axis_size("rep")
    n = ndom * nrep
    cores = 2
    row_tiles, kl, tile, _ = adj_local.shape
    kh = adj_halo.shape[1]
    rows, width = hop_feats.shape[1:]
    slots = train_ids.shape[1]
    hidden_units, classes = w_second.shape[0] * nrep, w_second.shape[1]
    chunk = slots // n
    block = 256
    steps = slots // block
    groups = block // chunk
    wide = -(-n // 128) * 128
    big = pltpu.CompilerParams(vmem_limit_bytes=BIG)
    sds = jax.ShapeDtypeStruct

    core = lax.rem(lax.axis_index("dom"), cores)
    own_cols = hidden_units // nrep
    h1, h2 = w_first.shape[0] // cores, w_second.shape[0] // cores
    half = jnp.concatenate([
        lax.dynamic_slice(w_first, (core * h1, 0), (h1, own_cols)),
        jnp.pad(lax.dynamic_slice(w_second, (core * h2, 0), (h2, classes)),
                ((0, 0), (0, own_cols - classes)))], axis=0)
    arrived = send_rep(half, nrep)

    sent_block = boundary_rows.shape[1] // steps
    x3, tags, sent, own_counts = pl.pallas_call(
        functools.partial(pick_kernel, chunk),
        out_shape=(sds((slots, 3 * width), BF16), sds((slots, 128), F32),
                   sds((boundary_rows.shape[1], width), BF16), sds((1, wide), F32)),
        grid=(steps,),
        in_specs=[lead_spec((block, 1)), lead_spec((sent_block, 1)), whole_spec((1, slots)),
                  whole_spec((1, rows)), whole_spec((1, rows)), whole_spec(hop_feats.shape)],
        out_specs=(lead_spec((block, 3 * width)), lead_spec((block, 128)),
                   lead_spec((sent_block, width)), whole_spec((1, wide))),
        compiler_params=big, name="pick",
        cost_estimate=pl.CostEstimate(flops=2 * slots * rows * 5 * width, bytes_accessed=4 << 20, transcendentals=0),
    )(shuffle[0][:, None], boundary_rows[0][:, None], train_ids, labels[None], labelled[None], hop_feats)

    arrived, own_counts = lax.optimization_barrier((arrived, own_counts))
    both = gather_rep(half, arrived, ndom, nrep, cores)
    sent = sent.reshape(n, -1, width)
    halo, counts = comm_call(
        functools.partial(halo_kernel, ndom, nrep), (sds(sent.shape, BF16), sds((1, wide), F32)),
        [pltpu.VMEM(sent.shape, BF16), pltpu.VMEM((1, 1, wide), F32), pltpu.VMEM((n, 1, wide), F32)]
        + dma_sems(n, 4), "halo", 1, sent, own_counts)
    halo = halo.reshape(-1, tile, width)

    next_hop = pl.pallas_call(
        functools.partial(hop_kernel, kl, kh),
        out_shape=sds((row_tiles, tile, width), BF16),
        grid=(row_tiles,),
        in_specs=[
            pl.BlockSpec(memory_space=pltpu.SMEM), pl.BlockSpec(memory_space=pltpu.SMEM),
            lead_spec((1, kl, tile, tile)), lead_spec((1, kh, tile, tile)),
            pl.BlockSpec((1, row_tiles, tile, width), lambda i: (2, 0, 0, 0)), whole_spec(halo.shape)],
        out_specs=lead_spec((1, tile, width)),
        compiler_params=big, name="hop",
        cost_estimate=pl.CostEstimate(flops=2 * rows * width * tile * (kl + kh), bytes_accessed=9 << 20, transcendentals=0),
    )(local_cols, halo_cols, adj_local, adj_halo, hop_feats.reshape(3, row_tiles, tile, width), halo)
    next_hop = next_hop.reshape(rows, width)

    w1 = both[:, :, :h1].transpose(1, 0, 2, 3).reshape(nrep, cores * h1, own_cols)
    w2 = both[:, :, h1:, :classes].transpose(1, 0, 2, 3).reshape(hidden_units, classes)

    lines = 2 * hidden_units // 128
    x, z, stats = pl.pallas_call(
        functools.partial(pre_kernel, chunk),
        out_shape=(sds((slots, 4 * width), BF16), sds((slots, hidden_units), F32),
                   sds((n, lines, 128), F32)),
        grid=(steps,),
        in_specs=[lead_spec((block, 3 * width)), lead_spec((block, 128)), whole_spec((rows, width)),
                  whole_spec(w1.shape)],
        out_specs=(lead_spec((block, 4 * width)), lead_spec((block, hidden_units)),
                   lead_spec((groups, lines, 128))),
        compiler_params=big, name="pre",
    )(x3, tags, next_hop, w1)

    def combine(values, row, forward, cid):
        return comm_call(
            functools.partial(stats_kernel, ndom, nrep, forward, chunk),
            (sds((n, lines, 128), F32), sds((1, wide), F32)),
            [pltpu.VMEM((n, lines, 128), F32)] * 2
            + [pltpu.VMEM((1, 1, wide), F32), pltpu.VMEM((n, 1, wide), F32)] + dma_sems(n, 6),
            "stats_f" if forward else "stats_b", cid, values, row)

    stats, _ = combine(stats, own_counts, True, 2)

    line_spec = lead_spec((groups, lines, 128))
    dlogits, grad_two, gsums, losses = pl.pallas_call(
        functools.partial(head_kernel, chunk),
        out_shape=(sds((slots, classes), BF16), sds((hidden_units, classes), F32),
                   sds((n, lines, 128), F32), sds((1, wide), F32)),
        grid=(steps,),
        in_specs=[lead_spec((block, hidden_units)), lead_spec((block, 128)), line_spec,
                  whole_spec((1, wide)), whole_spec((1, wide)), whole_spec((hidden_units, classes))],
        out_specs=(lead_spec((block, classes)), whole_spec((hidden_units, classes)), line_spec,
                   whole_spec((1, wide))),
        compiler_params=big, name="head",
    )(z, tags, stats, counts, own_counts, w2)

    gmeans, turned = combine(gsums, losses, False, 3)
    loss = turned[:, :n]

    own_rows, part = 4 * width // ndom, hidden_units // n
    size = (nrep, own_rows + part, own_cols)
    packed = pl.pallas_call(
        functools.partial(tail_kernel, chunk, ndom, nrep, cores),
        out_shape=sds((cores, ndom // cores) + size, BF16),
        grid=(steps,),
        in_specs=[lead_spec((block, hidden_units)), lead_spec((block, 4 * width)), line_spec, line_spec,
                  whole_spec((hidden_units, classes)), lead_spec((block, classes)),
                  whole_spec((hidden_units, classes))],
        out_specs=whole_spec((cores, ndom // cores) + size),
        scratch_shapes=[pltpu.VMEM((4 * width, hidden_units), F32)],
        compiler_params=big, name="tail",
    )(z, x, stats, gmeans, w2, dlogits, grad_two)

    chips = ndom // cores
    first, second = comm_call(
        functools.partial(grads_kernel, ndom, nrep, cores, own_rows),
        (sds((own_rows, own_cols), F32), sds((ndom, part, own_cols), F32)),
        [pltpu.VMEM((chips,) + size, BF16), pltpu.VMEM((chips,) + size, BF16),
         pltpu.VMEM((chips - 1,) + size, BF16), pltpu.VMEM(size, BF16), pltpu.VMEM(size, F32),
         pltpu.VMEM((nrep - 1,) + size[1:], BF16), pltpu.VMEM((ndom, part, own_cols), F32)]
        + dma_sems(chips, 4) + dma_sems(nrep, 2) + dma_sems(ndom, 2),
        "grads", 4, packed)
    second = second.reshape(ndom * part, own_cols)[:, :classes]
    return (next_hop, loss, first, second)


def solution(mesh):
    both = ("dom", "rep")
    placed = (
        P(None, both, None), P(both, None, None, None), P(both, None), P(both, None, None, None),
        P(both, None), P(both, None), P(both, None), P(both, None), P(both), P(both),
        P(None, "rep"), P("rep", None),
    )
    return jax.shard_map(
        shards, mesh=mesh, in_specs=placed,
        out_specs=(P(both, None), P(both, None), P("dom", "rep"), P("rep", None)),
        check_vma=False,
    )
```
